32 devices in a mesh: mol: 8 (over y, x, core), grid: 4 (over z).
Axes of the slice: x: 2, y: 2, z: 4, core: 2. Of those that a mesh axis runs over, the one named last changes fastest.
Arguments:
- cells_start: int32 [65536], P('mol'), may hold values from 0 to 524287
- moves: int32 [2, 3, 65536], P(None, None, 'mol'), may hold values from -1 to 1
- accepted: int32 [2, 65536], P(None, 'mol'), may hold values from 0 to 1
- bead_types: int32 [65536], P('mol'), may hold values from 0 to 1
Outputs:
- energy_change: float32 [2, 65536], P(None, 'mol')
- final_field: bfloat16 [64, 16, 1024], P('mol', 'grid')
The draws below stay inside these ranges and needn't reach their ends.
All inputs are finite; a program needn't handle non-finite values.
Results may differ from the reference program's by a relative error of at most 0.0048.
Values may be sent and summed in bfloat16 or wider, within the bound.
A program may use at most 64 MiB of HBM per device.

```python
import jax
import jax.numpy as jnp

NX = 512
NY = 64
STEPS = 2
TYPES = 2
SPREAD = 2
NZ = 16
BEADS = 65536
CELLS = 524288


def place_ends(array, rng, least, largest):
    spot = [jax.random.randint(jax.random.fold_in(rng, axis), (), 0, length) for axis, length in enumerate(array.shape)]
    longest = array.shape.index(max(array.shape))
    beside = spot[:longest] + [(spot[longest] + 1) % array.shape[longest]] + spot[longest + 1:]
    return array.at[tuple(spot)].set(least).at[tuple(beside)].set(largest)


def setup_inputs(seed: int = 0) -> dict:
    keys = jax.random.split(jax.random.key(seed), 5)
    cells_start = place_ends(jax.random.randint(keys[0], (BEADS,), 0, CELLS), jax.random.fold_in(keys[0], 1), 0, CELLS - 1).astype(jnp.int32)
    moves = place_ends(jax.random.randint(keys[1], (STEPS, 3, BEADS), -1, 2), jax.random.fold_in(keys[1], 1), -1, 1).astype(jnp.int32)
    accepted = place_ends(jax.random.randint(keys[2], (STEPS, BEADS), 0, 2), jax.random.fold_in(keys[2], 1), 0, 1).astype(jnp.int32)
    bead_types = place_ends(jax.random.randint(keys[3], (BEADS,), 0, TYPES), jax.random.fold_in(keys[3], 1), 0, TYPES - 1).astype(jnp.int32)
    return dict(cells_start=cells_start, moves=moves, accepted=accepted, bead_types=bead_types)


chi_mix = 1.0
kappa_comp = 0.5


def kernel_table():
    column = jnp.arange(NX, dtype=jnp.float32)
    distance = jnp.abs(column[:, None] - column[None, :])
    distance = jnp.minimum(distance, NX - distance)
    weights = jnp.exp(-distance * distance / (2.0 * SPREAD * SPREAD))
    first = jnp.abs(column)
    first = jnp.minimum(first, NX - first)
    total = jnp.sum(jnp.exp(-first * first / (2.0 * SPREAD * SPREAD)))
    return (weights / total).astype(jnp.bfloat16)


def split_cell(cells):
    col_x = cells % NX
    row_y = (cells // NX) % NY
    plane_z = cells // (NX * NY)
    return col_x, row_y, plane_z


def move_cells(cells, shift):
    col_x, row_y, plane_z = split_cell(cells)
    col_x = (col_x + shift[0]) % NX
    row_y = (row_y + shift[1]) % NY
    plane_z = (plane_z + shift[2]) % NZ
    return ((plane_z * NY + row_y) * NX + col_x).astype(jnp.int32)


def deposit(positions, bead_types, kernel):
    col_x, row_y, plane_z = split_cell(positions)
    rows = kernel[col_x].astype(jnp.float32)
    first = jnp.where(bead_types[:, None] == 0, rows, 0.0)
    second = jnp.where(bead_types[:, None] == 1, rows, 0.0)
    spread_rows = jnp.concatenate([first, second], axis=1)
    segment = (row_y * NZ + plane_z).astype(jnp.int32)
    summed = jax.ops.segment_sum(spread_rows, segment, num_segments=NY * NZ)
    scale = NX * NY * NZ / BEADS
    return (scale * summed).reshape(NY, NZ, 2 * NX)


def make_field(density):
    phi_a = density[:, :, :NX]
    phi_b = density[:, :, NX:]
    excess = kappa_comp * (phi_a + phi_b - 1.0)
    field_a = chi_mix * phi_b + excess
    field_b = chi_mix * phi_a + excess
    return jnp.concatenate([field_a, field_b], axis=2).astype(jnp.bfloat16)


def read_field(field, cells, bead_types):
    col_x, row_y, plane_z = split_cell(cells)
    flat_index = ((row_y * NZ + plane_z) * 2 + bead_types) * NX + col_x
    return jnp.take(field.reshape(-1), flat_index.astype(jnp.int32)).astype(jnp.float32)


def reference(cells_start, moves, accepted, bead_types):
    kernel = kernel_table()
    positions = cells_start
    changes = []
    field = None
    for step in range(STEPS):
        proposed = move_cells(positions, moves[step])
        field = make_field(deposit(positions, bead_types, kernel))
        changes.append(read_field(field, proposed, bead_types) - read_field(field, positions, bead_types))
        positions = jnp.where(accepted[step] == 1, proposed, positions)
    return jnp.stack(changes), field
```

```python
import functools

import jax
import jax.numpy as jnp
import numpy as np
from jax import lax
from jax.experimental import pallas as pl
from jax.experimental.pallas import tpu as pltpu
from jax.sharding import PartitionSpec as P

NX = 512
NY = 64
ZDEV = 4
STEPS = 2
TYPES = 2
SPREAD = 2

chi_mix = 1.0
kappa_comp = 0.5

MESH = pl.DeviceIdType.MESH
VMEM = pltpu.MemorySpace.VMEM
LIMIT = 60 * 1024 * 1024


def kernel_table():
    column = np.arange(NX, dtype=np.float32)
    distance = np.abs(column[:, None] - column[None, :])
    distance = np.minimum(distance, NX - distance)
    weights = np.exp(-distance * distance / np.float32(2.0 * SPREAD * SPREAD))
    return (weights / np.sum(weights[0])).astype(jnp.bfloat16)


def split_cell(cells):
    return cells % NX, cells // NX % NY, cells // (NX * NY)


def onehot(ids, size):
    tile = min(256, size)
    count = lax.broadcasted_iota(jnp.int32, (tile, ids.shape[1]), 0).astype(jnp.bfloat16)
    one = jnp.ones(count.shape, jnp.bfloat16)
    zero = jnp.zeros(count.shape, jnp.bfloat16)
    tiles = []
    for start in range(0, size, tile):
        here = jnp.broadcast_to((ids - start).astype(jnp.bfloat16), count.shape)
        tiles.append(jnp.where(count == here, one, zero))
    return jnp.concatenate(tiles, axis=0) if len(tiles) > 1 else tiles[0]


def deposit_kernel(row_ref, col_ref, out_ref, total):
    block = pl.program_id(1)

    @pl.when(block == 0)
    def _():
        total[...] = jnp.zeros_like(total)

    rows = onehot(row_ref[0], total.shape[0])
    cols = onehot(col_ref[0], total.shape[1])
    total[...] += lax.dot_general(
        rows, cols, (((1,), (1,)), ((), ())), preferred_element_type=jnp.float32
    )

    @pl.when(block == pl.num_programs(1) - 1)
    def _():
        out_ref[0] = total[...].astype(jnp.bfloat16)


def deposit(rows, cols, row_total):
    beads = rows.shape[-1]
    block = min(1024, beads)
    return pl.pallas_call(
        deposit_kernel,
        grid=(STEPS, beads // block),
        out_shape=jax.ShapeDtypeStruct((STEPS, row_total, NX), jnp.bfloat16),
        in_specs=[pl.BlockSpec((1, 1, block), lambda s, b: (s, 0, b))] * 2,
        out_specs=pl.BlockSpec((1, row_total, NX), lambda s, b: (s, 0, 0)),
        scratch_shapes=[pltpu.VMEM((row_total, NX), jnp.float32)],
        compiler_params=pltpu.CompilerParams(vmem_limit_bytes=LIMIT),
        name="deposit",
    )(rows, cols)


def field_kernel(peers, scale, count_ref, table_ref, all_ref, own_ref, inbox, sums, send_a, recv_a, send_b, recv_b):
    me = lax.axis_index("mol")
    barrier = pltpu.get_barrier_semaphore()
    for away in range(1, peers):
        pl.semaphore_signal(
            barrier, inc=1, device_id={"mol": lax.rem(me + away, peers)}, device_id_type=MESH
        )
    pl.semaphore_wait(barrier, peers - 1)
    parts = {}
    for step in range(STEPS):
        for away in range(1, peers):
            to = lax.rem(me + away, peers)
            copy = pltpu.make_async_remote_copy(
                src_ref=count_ref.at[step, to],
                dst_ref=inbox.at[step, away - 1],
                send_sem=send_a.at[step, away - 1],
                recv_sem=recv_a.at[step, away - 1],
                device_id={"mol": to},
                device_id_type=MESH,
            )
            copy.start()
            parts[step, away] = copy
    half = count_ref.shape[2] // 2
    fields = {}
    for step in range(STEPS):
        total = count_ref[step, me].astype(jnp.float32)
        for away in range(1, peers):
            parts[step, away].wait_recv()
            total = total + inbox[step, away - 1].astype(jnp.float32)
        sums[...] = total
        high = sums[...].astype(jnp.bfloat16)
        low = (sums[...] - high.astype(jnp.float32)).astype(jnp.bfloat16)
        table = table_ref[...]
        density = jnp.dot(high, table, preferred_element_type=jnp.float32)
        density = scale * (density + jnp.dot(low, table, preferred_element_type=jnp.float32))
        phi_a, phi_b = density[:half], density[half:]
        excess = kappa_comp * (phi_a + phi_b - 1.0)
        field_a = (chi_mix * phi_b + excess).astype(jnp.bfloat16)
        field_b = (chi_mix * phi_a + excess).astype(jnp.bfloat16)
        all_ref[step, me, :half] = field_a
        all_ref[step, me, half:] = field_b
        if step == STEPS - 1:
            own_ref[:, :NX] = field_a
            own_ref[:, NX:] = field_b
        for away in range(1, peers):
            to = lax.rem(me + away, peers)
            copy = pltpu.make_async_remote_copy(
                src_ref=all_ref.at[step, me],
                dst_ref=all_ref.at[step, me],
                send_sem=send_b.at[step, away - 1],
                recv_sem=recv_b.at[step, away - 1],
                device_id={"mol": to},
                device_id_type=MESH,
            )
            copy.start()
            fields[step, away] = copy
    for step in range(STEPS):
        for away in range(1, peers):
            fields[step, away].wait_recv()
    for step in range(STEPS):
        for away in range(1, peers):
            parts[step, away].wait_send()
            fields[step, away].wait_send()


def make_fields(counts, table, scale):
    steps, peers, rows, _ = counts.shape
    spec = pl.BlockSpec(memory_space=VMEM)
    sems = [pltpu.SemaphoreType.DMA((steps, peers - 1))] * 4
    return pl.pallas_call(
        functools.partial(field_kernel, peers, scale),
        out_shape=[
            jax.ShapeDtypeStruct(counts.shape, jnp.bfloat16),
            jax.ShapeDtypeStruct((rows // TYPES, TYPES * NX), jnp.bfloat16),
        ],
        in_specs=[spec] * 2,
        out_specs=[spec] * 2,
        scratch_shapes=[
            pltpu.VMEM((steps, peers - 1, rows, NX), jnp.bfloat16),
            pltpu.VMEM((rows, NX), jnp.float32),
            *sems,
        ],
        compiler_params=pltpu.CompilerParams(
            collective_id=0, has_side_effects=True, vmem_limit_bytes=LIMIT
        ),
        name="fields",
    )(counts, table)


def read_kernel(rc_ref, cc_ref, rp_ref, cp_ref, field_ref, out_ref, turned):
    @pl.when(pl.program_id(1) == 0)
    def _():
        size = turned.shape[0]
        eye = (
            lax.broadcasted_iota(jnp.int32, (size, size), 0)
            == lax.broadcasted_iota(jnp.int32, (size, size), 1)
        )
        eye = jnp.where(eye, 1.0, 0.0).astype(jnp.bfloat16)
        turned[...] = lax.dot_general(
            eye, field_ref[0], (((1,), (1,)), ((), ())), preferred_element_type=jnp.float32
        ).astype(jnp.bfloat16)

    table = turned[...]

    def pick(rows, cols):
        values = jnp.dot(table, onehot(rows, table.shape[1]), preferred_element_type=jnp.float32)
        columns = lax.broadcasted_iota(jnp.int32, values.shape, 0)
        return jnp.sum(jnp.where(columns == cols, values, 0.0), axis=0, keepdims=True)

    out_ref[0] = pick(rp_ref[0], cp_ref[0]) - pick(rc_ref[0], cc_ref[0])


def read(rows, cols, rows_p, cols_p, field):
    beads = rows.shape[-1]
    block = min(1024, beads)
    spec = pl.BlockSpec((1, 1, block), lambda s, b: (s, 0, b))
    row_total = field.shape[1]
    return pl.pallas_call(
        read_kernel,
        grid=(STEPS, beads // block),
        out_shape=jax.ShapeDtypeStruct((STEPS, 1, beads), jnp.float32),
        in_specs=[spec] * 4 + [pl.BlockSpec((1, row_total, NX), lambda s, b: (s, 0, 0))],
        out_specs=spec,
        scratch_shapes=[pltpu.VMEM((NX, row_total), jnp.bfloat16)],
        compiler_params=pltpu.CompilerParams(vmem_limit_bytes=LIMIT),
        name="read",
    )(rows, cols, rows_p, cols_p, field)


def exchange_kernel(peers, part_ref, out_ref, inbox, send, recv):
    me = lax.axis_index("grid")
    barrier = pltpu.get_barrier_semaphore()
    for away in range(1, peers):
        pl.semaphore_signal(
            barrier, inc=1, device_id={"grid": lax.rem(me + away, peers)}, device_id_type=MESH
        )
    pl.semaphore_wait(barrier, peers - 1)
    copies = []
    for away in range(1, peers):
        copy = pltpu.make_async_remote_copy(
            src_ref=part_ref,
            dst_ref=inbox.at[away - 1],
            send_sem=send.at[away - 1],
            recv_sem=recv.at[away - 1],
            device_id={"grid": lax.rem(me + away, peers)},
            device_id_type=MESH,
        )
        copy.start()
        copies.append(copy)
    total = part_ref[...]
    for away in range(1, peers):
        copies[away - 1].wait_recv()
        total = total + inbox[away - 1]
    out_ref[...] = total
    for copy in copies:
        copy.wait_send()


def exchange(part, peers):
    spec = pl.BlockSpec(memory_space=VMEM)
    return pl.pallas_call(
        functools.partial(exchange_kernel, peers),
        out_shape=jax.ShapeDtypeStruct(part.shape, jnp.float32),
        in_specs=[spec],
        out_specs=spec,
        scratch_shapes=[
            pltpu.VMEM((peers - 1, *part.shape), jnp.float32),
            pltpu.SemaphoreType.DMA((peers - 1,)),
            pltpu.SemaphoreType.DMA((peers - 1,)),
        ],
        compiler_params=pltpu.CompilerParams(
            collective_id=1, has_side_effects=True, vmem_limit_bytes=LIMIT
        ),
        name="exchange",
    )(part)


def local(cells_start, moves, accepted, bead_types):
    grid_count = lax.axis_size("grid")
    mol_count = lax.axis_size("mol")
    slab = lax.axis_index("grid")
    planes = ZDEV * grid_count
    beads = cells_start.shape[0]
    scale = NX * NY * planes / (beads * mol_count)
    band = NY // mol_count
    row_total = TYPES * NY * ZDEV

    def row_of(spot):
        _, row_y, plane_z = spot
        inside = plane_z // ZDEV == slab
        row = ((row_y // band * TYPES + bead_types) * band + row_y % band) * ZDEV
        return jnp.where(inside, row + plane_z % ZDEV, -1)

    position = split_cell(cells_start)
    spots, proposals = [], []
    for step in range(STEPS):
        lengths = (NX, NY, planes)
        proposed = tuple((position[i] + moves[step, i]) % lengths[i] for i in range(3))
        spots.append(position)
        proposals.append(proposed)
        position = tuple(
            jnp.where(accepted[step] == 1, proposed[i], position[i]) for i in range(3)
        )
    rows = jnp.stack([row_of(spot) for spot in spots])[:, None]
    cols = jnp.stack([spot[0] for spot in spots])[:, None]
    rows_p = jnp.stack([row_of(spot) for spot in proposals])[:, None]
    cols_p = jnp.stack([spot[0] for spot in proposals])[:, None]

    counts = deposit(rows, cols, row_total)
    counts = counts.reshape(STEPS, mol_count, row_total // mol_count, NX)
    fields, own = make_fields(counts, jnp.asarray(kernel_table()), scale)
    part = read(rows, cols, rows_p, cols_p, fields.reshape(STEPS, row_total, NX))
    part = part.reshape(-1, 128)
    total = exchange(part, grid_count).reshape(STEPS, beads)
    return total, own.reshape(band, ZDEV, TYPES * NX)


def solution(mesh):
    return jax.shard_map(
        local,
        mesh=mesh,
        in_specs=(P("mol"), P(None, None, "mol"), P(None, "mol"), P("mol")),
        out_specs=(P(None, "mol"), P("mol", "grid", None)),
        check_vma=False,
    )
```

```python
import functools

import jax
import jax.numpy as jnp
import numpy as np
from jax import lax
from jax.experimental import pallas as pl
from jax.experimental.pallas import tpu as pltpu
from jax.sharding import PartitionSpec as P

NX = 512
NY = 64
ZDEV = 4
STEPS = 2
TYPES = 2
SPREAD = 2

chi_mix = 1.0
kappa_comp = 0.5

MESH = pl.DeviceIdType.MESH
VMEM = pltpu.MemorySpace.VMEM
LIMIT = 60 * 1024 * 1024


def kernel_table():
    column = np.arange(NX, dtype=np.float32)
    distance = np.abs(column[:, None] - column[None, :])
    distance = np.minimum(distance, NX - distance)
    weights = np.exp(-distance * distance / np.float32(2.0 * SPREAD * SPREAD))
    return (weights / np.sum(weights[0])).astype(jnp.bfloat16)


def split_cell(cells):
    return cells % NX, cells // NX % NY, cells // (NX * NY)


def onehot(ids, size):
    tile = min(256, size)
    count = lax.broadcasted_iota(jnp.int32, (tile, ids.shape[1]), 0).astype(jnp.bfloat16)
    one = jnp.ones(count.shape, jnp.bfloat16)
    zero = jnp.zeros(count.shape, jnp.bfloat16)
    tiles = []
    for start in range(0, size, tile):
        here = jnp.broadcast_to((ids - start).astype(jnp.bfloat16), count.shape)
        tiles.append(jnp.where(count == here, one, zero))
    return jnp.concatenate(tiles, axis=0) if len(tiles) > 1 else tiles[0]


def fused_kernel(
    mol, grid, scale, cell_ref, move_ref, accept_ref, type_ref, table_ref,
    out_ref, own_ref,
    ids, total, count, inbox, fields, turned, part, inbox_e,
    send_a, recv_a, send_b, recv_b, send_e, recv_e,
):
    me = lax.axis_index("mol")
    slab = lax.axis_index("grid")
    beads = cell_ref.shape[1]
    blocks, block = part.shape[1], part.shape[3]
    planes = ZDEV * grid
    band = NY // mol
    half = count.shape[2] // 2

    barrier = pltpu.get_barrier_semaphore()
    for away in range(1, mol):
        pl.semaphore_signal(
            barrier, inc=1, device_id={"mol": lax.rem(me + away, mol)}, device_id_type=MESH
        )
    for away in range(1, grid):
        pl.semaphore_signal(
            barrier, inc=1, device_id={"grid": lax.rem(slab + away, grid)}, device_id_type=MESH
        )

    def window(index):
        return pl.ds(pl.multiple_of(index * block, block), block)

    def row_of(spot, kinds):
        _, row_y, plane_z = spot
        row = ((row_y // band * TYPES + kinds) * band + row_y % band) * ZDEV + plane_z % ZDEV
        return jnp.where(plane_z // ZDEV == slab, row, -1)

    def wrap(value, length):
        value = jnp.where(value < 0, value + length, value)
        return jnp.where(value >= length, value - length, value)

    def prepare(index, carry):
        here = window(index)
        kinds = type_ref[:, here]
        position = split_cell(cell_ref[:, here])
        for step in range(STEPS):
            lengths = (NX, NY, planes)
            proposed = tuple(
                wrap(position[i] + move_ref[step, i : i + 1, here], lengths[i]) for i in range(3)
            )
            ids[4 * step, :, here] = row_of(position, kinds)
            ids[4 * step + 1, :, here] = position[0]
            ids[4 * step + 2, :, here] = row_of(proposed, kinds)
            ids[4 * step + 3, :, here] = proposed[0]
            taken = accept_ref[step : step + 1, here] == 1
            position = tuple(jnp.where(taken, proposed[i], position[i]) for i in range(3))
        return carry

    lax.fori_loop(0, blocks, prepare, 0)

    def deposit(step, begin, end):
        def add(index, carry):
            here = window(index)
            rows = onehot(ids[4 * step, :, here], total.shape[0])
            cols = onehot(ids[4 * step + 1, :, here], total.shape[1])
            total[...] += lax.dot_general(
                rows, cols, (((1,), (1,)), ((), ())), preferred_element_type=jnp.float32
            )
            return carry

        if begin == 0:
            total[...] = jnp.zeros_like(total)
        lax.fori_loop(begin, end, add, 0)
        if end == blocks:
            count[step] = total[...].astype(jnp.bfloat16).reshape(count.shape[1:])

    def copy_a(step, away):
        to = lax.rem(me + away, mol)
        return pltpu.make_async_remote_copy(
            src_ref=count.at[step, to],
            dst_ref=inbox.at[step, away - 1],
            send_sem=send_a.at[step, away - 1],
            recv_sem=recv_a.at[step, away - 1],
            device_id={"mol": to},
            device_id_type=MESH,
        )

    def copy_b(step, away):
        return pltpu.make_async_remote_copy(
            src_ref=fields.at[step, me],
            dst_ref=fields.at[step, me],
            send_sem=send_b.at[step, away - 1],
            recv_sem=recv_b.at[step, away - 1],
            device_id={"mol": lax.rem(me + away, mol)},
            device_id_type=MESH,
        )

    def copy_e(step, index, away):
        return pltpu.make_async_remote_copy(
            src_ref=part.at[step, index],
            dst_ref=inbox_e.at[away - 1, step, index],
            send_sem=send_e.at[step, index, away - 1],
            recv_sem=recv_e.at[step, index, away - 1],
            device_id={"grid": lax.rem(slab + away, grid)},
            device_id_type=MESH,
        )

    def make_field(step):
        summed = count[step, me].astype(jnp.float32)
        for away in range(1, mol):
            copy_a(step, away).wait_recv()
            summed = summed + inbox[step, away - 1].astype(jnp.float32)
        high = summed.astype(jnp.bfloat16)
        low = (summed - high.astype(jnp.float32)).astype(jnp.bfloat16)
        table = table_ref[...]
        density = jnp.dot(high, table, preferred_element_type=jnp.float32)
        density = scale * (density + jnp.dot(low, table, preferred_element_type=jnp.float32))
        phi_a, phi_b = density[:half], density[half:]
        excess = kappa_comp * (phi_a + phi_b - 1.0)
        field_a = (chi_mix * phi_b + excess).astype(jnp.bfloat16)
        field_b = (chi_mix * phi_a + excess).astype(jnp.bfloat16)
        fields[step, me, :half] = field_a
        fields[step, me, half:] = field_b
        for away in range(1, mol):
            copy_b(step, away).start()
        if step == STEPS - 1:
            own_ref[:, :NX] = field_a
            own_ref[:, NX:] = field_b

    def turn(step):
        for away in range(1, mol):
            copy_b(step, away).wait_recv()
        eye = (
            lax.broadcasted_iota(jnp.int32, (NX, NX), 0)
            == lax.broadcasted_iota(jnp.int32, (NX, NX), 1)
        )
        eye = jnp.where(eye, 1.0, 0.0).astype(jnp.bfloat16)
        flat = fields[step].reshape(turned.shape[1], NX)
        turned[...] = lax.dot_general(
            eye, flat, (((1,), (1,)), ((), ())), preferred_element_type=jnp.float32
        ).astype(jnp.bfloat16)

    def pick(rows, cols):
        table = turned[...]
        values = jnp.dot(table, onehot(rows, table.shape[1]), preferred_element_type=jnp.float32)
        columns = lax.broadcasted_iota(jnp.int32, values.shape, 0)
        return jnp.sum(jnp.where(columns == cols, values, 0.0), axis=0, keepdims=True)

    def read(step, begin, end):
        def look(index, carry):
            here = window(index)
            old = pick(ids[4 * step, :, here], ids[4 * step + 1, :, here])
            new = pick(ids[4 * step + 2, :, here], ids[4 * step + 3, :, here])
            part[step, index] = new - old
            for away in range(1, grid):
                copy_e(step, index, away).start()
            return carry

        lax.fori_loop(begin, end, look, 0)

    deposit(0, 0, blocks)
    pl.semaphore_wait(barrier, mol - 1 + grid - 1)
    for away in range(1, mol):
        copy_a(0, away).start()
    early = blocks * 3 // 4
    deposit(1, 0, early)
    make_field(0)
    deposit(1, early, blocks)
    for away in range(1, mol):
        copy_a(1, away).start()
    turn(0)
    middle = blocks // 2
    read(0, 0, middle)
    make_field(1)
    read(0, middle, blocks)
    turn(1)
    read(1, 0, blocks)

    for step in range(STEPS):
        def settle(index, carry):
            energy = part[step, index]
            for away in range(1, grid):
                copy_e(step, index, away).wait_recv()
                energy = energy + inbox_e[away - 1, step, index]
            out_ref[step : step + 1, window(index)] = energy
            return carry

        lax.fori_loop(0, blocks, settle, 0)
    for step in range(STEPS):
        for away in range(1, mol):
            copy_a(step, away).wait_send()
            copy_b(step, away).wait_send()

        def drain(index, carry):
            for away in range(1, grid):
                copy_e(step, index, away).wait_send()
            return carry

        lax.fori_loop(0, blocks, drain, 0)


def local(cells_start, moves, accepted, bead_types):
    grid = lax.axis_size("grid")
    mol = lax.axis_size("mol")
    planes = ZDEV * grid
    beads = cells_start.shape[0]
    scale = NX * NY * planes / (beads * mol)
    band = NY // mol
    row_total = TYPES * NY * ZDEV
    rows = row_total // mol
    block = min(1024, beads)
    blocks = beads // block
    spec = pl.BlockSpec(memory_space=VMEM)
    bf16, f32 = jnp.bfloat16, jnp.float32
    dma = pltpu.SemaphoreType.DMA
    total, own = pl.pallas_call(
        functools.partial(fused_kernel, mol, grid, scale),
        out_shape=[
            jax.ShapeDtypeStruct((STEPS, beads), f32),
            jax.ShapeDtypeStruct((band * ZDEV, TYPES * NX), bf16),
        ],
        in_specs=[spec] * 5,
        out_specs=[spec] * 2,
        scratch_shapes=[
            pltpu.VMEM((4 * STEPS, 1, beads), jnp.int32),
            pltpu.VMEM((row_total, NX), f32),
            pltpu.VMEM((STEPS, mol, rows, NX), bf16),
            pltpu.VMEM((STEPS, mol - 1, rows, NX), bf16),
            pltpu.VMEM((STEPS, mol, rows, NX), bf16),
            pltpu.VMEM((NX, row_total), bf16),
            pltpu.VMEM((STEPS, blocks, 1, block), f32),
            pltpu.VMEM((grid - 1, STEPS, blocks, 1, block), f32),
            dma((STEPS, mol - 1)),
            dma((STEPS, mol - 1)),
            dma((STEPS, mol - 1)),
            dma((STEPS, mol - 1)),
            dma((STEPS, blocks, grid - 1)),
            dma((STEPS, blocks, grid - 1)),
        ],
        compiler_params=pltpu.CompilerParams(
            collective_id=0, has_side_effects=True, vmem_limit_bytes=LIMIT
        ),
        name="chain",
    )(
        cells_start.reshape(1, beads), moves, accepted,
        bead_types.reshape(1, beads), jnp.asarray(kernel_table()),
    )
    return total, own.reshape(band, ZDEV, TYPES * NX)


def solution(mesh):
    return jax.shard_map(
        local,
        mesh=mesh,
        in_specs=(P("mol"), P(None, None, "mol"), P(None, "mol"), P("mol")),
        out_specs=(P(None, "mol"), P("mol", "grid", None)),
        check_vma=False,
    )
```

```python
import functools

import jax
import jax.numpy as jnp
import numpy as np
from jax import lax
from jax.experimental import pallas as pl
from jax.experimental.pallas import tpu as pltpu
from jax.sharding import PartitionSpec as P

NX = 512
NY = 64
ZDEV = 4
STEPS = 2
TYPES = 2
SPREAD = 2

chi_mix = 1.0
kappa_comp = 0.5

MESH = pl.DeviceIdType.MESH
VMEM = pltpu.MemorySpace.VMEM
LIMIT = 60 * 1024 * 1024


def kernel_table():
    column = np.arange(NX, dtype=np.float32)
    distance = np.abs(column[:, None] - column[None, :])
    distance = np.minimum(distance, NX - distance)
    weights = np.exp(-distance * distance / np.float32(2.0 * SPREAD * SPREAD))
    return (weights / np.sum(weights[0])).astype(jnp.bfloat16)


def divide(value, size):
    if size & (size - 1) == 0:
        return value >> (size.bit_length() - 1), value & (size - 1)
    return value // size, value % size


def split_cell(cells):
    rest, col_x = divide(cells, NX)
    plane_z, row_y = divide(rest, NY)
    return col_x, row_y, plane_z


def onehot(ids, size):
    tile = min(256, size)
    count = lax.broadcasted_iota(jnp.int32, (tile, ids.shape[1]), 0).astype(jnp.bfloat16)
    one = jnp.ones(count.shape, jnp.bfloat16)
    zero = jnp.zeros(count.shape, jnp.bfloat16)
    tiles = []
    for start in range(0, size, tile):
        here = jnp.broadcast_to((ids - start).astype(jnp.bfloat16), count.shape)
        tiles.append(jnp.where(count == here, one, zero))
    return jnp.concatenate(tiles, axis=0) if len(tiles) > 1 else tiles[0]


def fused_kernel(
    mol, grid, scale, cell_ref, move_ref, accept_ref, type_ref, table_ref,
    out_ref, own_ref,
    ids, total, count, inbox, fields, turned, part, inbox_e,
    send_a, recv_a, send_b, recv_b, send_e, recv_e,
):
    me = lax.axis_index("mol")
    slab = lax.axis_index("grid")
    beads = cell_ref.shape[1]
    blocks, block = part.shape[1], part.shape[3]
    planes = ZDEV * grid
    band = NY // mol
    half = count.shape[2] // 2

    barrier = pltpu.get_barrier_semaphore()
    for away in range(1, mol):
        pl.semaphore_signal(
            barrier, inc=1, device_id={"mol": lax.rem(me + away, mol)}, device_id_type=MESH
        )
    for away in range(1, grid):
        pl.semaphore_signal(
            barrier, inc=1, device_id={"grid": lax.rem(slab + away, grid)}, device_id_type=MESH
        )

    def window(index):
        return pl.ds(pl.multiple_of(index * block, block), block)

    def row_of(spot, kinds):
        _, row_y, plane_z = spot
        owner, row_here = divide(row_y, band)
        owner_z, plane_here = divide(plane_z, ZDEV)
        row = ((owner * TYPES + kinds) * band + row_here) * ZDEV + plane_here
        return jnp.where(owner_z == slab, row, -1)

    def wrap(value, length):
        value = jnp.where(value < 0, value + length, value)
        return jnp.where(value >= length, value - length, value)

    def begin_ids(index, carry):
        here = window(index)
        position = split_cell(cell_ref[:, here])
        ids[0, :, here] = row_of(position, type_ref[:, here])
        ids[1, :, here] = position[0]
        return carry

    def prepare(index, carry):
        here = window(index)
        kinds = type_ref[:, here]
        position = split_cell(cell_ref[:, here])
        for step in range(STEPS):
            lengths = (NX, NY, planes)
            proposed = tuple(
                wrap(position[i] + move_ref[i, step : step + 1, here], lengths[i]) for i in range(3)
            )
            if step > 0:
                ids[4 * step, :, here] = row_of(position, kinds)
                ids[4 * step + 1, :, here] = position[0]
            ids[4 * step + 2, :, here] = row_of(proposed, kinds)
            ids[4 * step + 3, :, here] = proposed[0]
            taken = accept_ref[step : step + 1, here] == 1
            position = tuple(jnp.where(taken, proposed[i], position[i]) for i in range(3))
        return carry

    lax.fori_loop(0, blocks, begin_ids, 0)

    def deposit(step, begin, end):
        def add(index, carry):
            here = window(index)
            rows = onehot(ids[4 * step, :, here], total.shape[0]).astype(jnp.float8_e4m3fn)
            cols = onehot(ids[4 * step + 1, :, here], total.shape[1]).astype(jnp.float8_e4m3fn)
            total[...] += lax.dot_general(
                rows, cols, (((1,), (1,)), ((), ())), preferred_element_type=jnp.float32
            )
            return carry

        if begin == 0:
            total[...] = jnp.zeros_like(total)
        lax.fori_loop(begin, end, add, 0)
        if end == blocks:
            count[step] = total[...].astype(jnp.bfloat16).reshape(count.shape[1:])

    def copy_a(step, away):
        to = lax.rem(me + away, mol)
        return pltpu.make_async_remote_copy(
            src_ref=count.at[step, to],
            dst_ref=inbox.at[step, away - 1],
            send_sem=send_a.at[step, away - 1],
            recv_sem=recv_a.at[step, away - 1],
            device_id={"mol": to},
            device_id_type=MESH,
        )

    partner = me + 1 - 2 * lax.rem(me, 2)
    chips = mol // 2

    def copy_b(step, index):
        if index == 0:
            slot, to = me, partner
        elif index < chips:
            slot, to = me, lax.rem(me + 2 * index, mol)
        else:
            slot, to = lax.rem(me + mol - 2 * (index - chips + 1), mol), partner
        return pltpu.make_async_remote_copy(
            src_ref=fields.at[step, slot],
            dst_ref=fields.at[step, slot],
            send_sem=send_b.at[step, index],
            recv_sem=recv_b.at[step, index],
            device_id={"mol": to},
            device_id_type=MESH,
        )

    def forward(step):
        for index in range(1, chips):
            copy_b(step, index).wait_recv()
            copy_b(step, index + chips - 1).start()

    def copy_e(step, index, away):
        return pltpu.make_async_remote_copy(
            src_ref=part.at[step, index],
            dst_ref=inbox_e.at[away - 1, step, index],
            send_sem=send_e.at[step, index, away - 1],
            recv_sem=recv_e.at[step, index, away - 1],
            device_id={"grid": lax.rem(slab + away, grid)},
            device_id_type=MESH,
        )

    def make_field(step):
        summed = count[step, me].astype(jnp.float32)
        for away in range(1, mol):
            copy_a(step, away).wait_recv()
            summed = summed + inbox[step, away - 1].astype(jnp.float32)
        high = summed.astype(jnp.bfloat16)
        low = (summed - high.astype(jnp.float32)).astype(jnp.bfloat16)
        table = table_ref[...]
        density = jnp.dot(high, table, preferred_element_type=jnp.float32)
        density = scale * (density + jnp.dot(low, table, preferred_element_type=jnp.float32))
        phi_a, phi_b = density[:half], density[half:]
        excess = kappa_comp * (phi_a + phi_b - 1.0)
        wide_a = chi_mix * phi_b + excess
        wide_b = chi_mix * phi_a + excess
        fields[step, me, :half] = wide_a.astype(jnp.bfloat16)
        fields[step, me, half:] = wide_b.astype(jnp.bfloat16)
        for index in reversed(range(chips)):
            copy_b(step, index).start()
        if step == STEPS - 1:
            for row in range(band):
                here = slice(row * ZDEV, (row + 1) * ZDEV)
                own_ref[row, :, :NX] = wide_a[here].astype(jnp.bfloat16)
                own_ref[row, :, NX:] = wide_b[here].astype(jnp.bfloat16)

    def turn(step):
        for index in [0, *range(chips, 2 * chips - 1)]:
            copy_b(step, index).wait_recv()
        eye = (
            lax.broadcasted_iota(jnp.int32, (NX, NX), 0)
            == lax.broadcasted_iota(jnp.int32, (NX, NX), 1)
        )
        eye = jnp.where(eye, 1.0, 0.0).astype(jnp.bfloat16)
        flat = fields[step].reshape(turned.shape[1], NX)
        turned[...] = lax.dot_general(
            eye, flat, (((1,), (1,)), ((), ())), preferred_element_type=jnp.float32
        ).astype(jnp.bfloat16)

    def pick(rows, cols):
        table = turned[...]
        values = jnp.dot(table, onehot(rows, table.shape[1]), preferred_element_type=jnp.float32)
        columns = lax.broadcasted_iota(jnp.int32, values.shape, 0)
        return jnp.sum(jnp.where(columns == cols, values, 0.0), axis=0, keepdims=True)

    def read(step, begin, end):
        def look(index, carry):
            here = window(index)
            old = pick(ids[4 * step, :, here], ids[4 * step + 1, :, here])
            new = pick(ids[4 * step + 2, :, here], ids[4 * step + 3, :, here])
            part[step, index] = new - old
            for away in range(1, grid):
                copy_e(step, index, away).start()
            return carry

        lax.fori_loop(begin, end, look, 0)

    deposit(0, 0, blocks)
    pl.semaphore_wait(barrier, mol - 1 + grid - 1)
    for away in range(1, mol):
        copy_a(0, away).start()
    lax.fori_loop(0, blocks, prepare, 0)
    deposit(1, 0, blocks)
    make_field(0)
    for away in range(1, mol):
        copy_a(1, away).start()
    forward(0)
    turn(0)
    middle, late = blocks // 2, blocks * 3 // 4
    read(0, 0, middle)
    make_field(1)
    read(0, middle, late)
    forward(1)
    read(0, late, blocks)
    turn(1)
    read(1, 0, blocks)

    for step in range(STEPS):
        def settle(index, carry):
            energy = part[step, index]
            for away in range(1, grid):
                copy_e(step, index, away).wait_recv()
                energy = energy + inbox_e[away - 1, step, index]
            out_ref[step : step + 1, window(index)] = energy
            return carry

        lax.fori_loop(0, blocks, settle, 0)
    for step in range(STEPS):
        for away in range(1, mol):
            copy_a(step, away).wait_send()
            copy_b(step, away - 1).wait_send()

        def drain(index, carry):
            for away in range(1, grid):
                copy_e(step, index, away).wait_send()
            return carry

        lax.fori_loop(0, blocks, drain, 0)


def local(cells_start, moves, accepted, bead_types):
    grid = lax.axis_size("grid")
    mol = lax.axis_size("mol")
    planes = ZDEV * grid
    beads = cells_start.shape[0]
    scale = NX * NY * planes / (beads * mol)
    band = NY // mol
    row_total = TYPES * NY * ZDEV
    rows = row_total // mol
    block = min(2048, beads)
    blocks = beads // block
    spec = pl.BlockSpec(memory_space=VMEM)
    bf16, f32 = jnp.bfloat16, jnp.float32
    dma = pltpu.SemaphoreType.DMA
    total, own = pl.pallas_call(
        functools.partial(fused_kernel, mol, grid, scale),
        out_shape=[
            jax.ShapeDtypeStruct((STEPS, beads), f32),
            jax.ShapeDtypeStruct((band, ZDEV, TYPES * NX), bf16),
        ],
        in_specs=[spec] * 5,
        out_specs=[spec] * 2,
        scratch_shapes=[
            pltpu.VMEM((4 * STEPS, 1, beads), jnp.int32),
            pltpu.VMEM((row_total, NX), f32),
            pltpu.VMEM((STEPS, mol, rows, NX), bf16),
            pltpu.VMEM((STEPS, mol - 1, rows, NX), bf16),
            pltpu.VMEM((STEPS, mol, rows, NX), bf16),
            pltpu.VMEM((NX, row_total), bf16),
            pltpu.VMEM((STEPS, blocks, 1, block), f32),
            pltpu.VMEM((grid - 1, STEPS, blocks, 1, block), f32),
            dma((STEPS, mol - 1)),
            dma((STEPS, mol - 1)),
            dma((STEPS, mol - 1)),
            dma((STEPS, mol - 1)),
            dma((STEPS, blocks, grid - 1)),
            dma((STEPS, blocks, grid - 1)),
        ],
        compiler_params=pltpu.CompilerParams(
            collective_id=0, has_side_effects=True, vmem_limit_bytes=LIMIT
        ),
        name="chain",
    )(
        cells_start.reshape(1, beads), moves.transpose(1, 0, 2), accepted,
        bead_types.reshape(1, beads), jnp.asarray(kernel_table()),
    )
    return total, own


def solution(mesh):
    return jax.shard_map(
        local,
        mesh=mesh,
        in_specs=(P("mol"), P(None, None, "mol"), P(None, "mol"), P("mol")),
        out_specs=(P(None, "mol"), P("mol", "grid", None)),
        check_vma=False,
    )
```

```python
import functools

import jax
import jax.numpy as jnp
import numpy as np
from jax import lax
from jax.experimental import pallas as pl
from jax.experimental.pallas import tpu as pltpu
from jax.sharding import PartitionSpec as P

NX = 512
NY = 64
ZDEV = 4
STEPS = 2
TYPES = 2
SPREAD = 2

chi_mix = 1.0
kappa_comp = 0.5

MESH = pl.DeviceIdType.MESH
VMEM = pltpu.MemorySpace.VMEM
LIMIT = 60 * 1024 * 1024


def kernel_table():
    column = np.arange(NX, dtype=np.float32)
    distance = np.abs(column[:, None] - column[None, :])
    distance = np.minimum(distance, NX - distance)
    weights = np.exp(-distance * distance / np.float32(2.0 * SPREAD * SPREAD))
    return (weights / np.sum(weights[0])).astype(jnp.bfloat16)


def divide(value, size):
    if size & (size - 1) == 0:
        return value >> (size.bit_length() - 1), value & (size - 1)
    return value // size, value % size


def split_cell(cells):
    rest, col_x = divide(cells, NX)
    plane_z, row_y = divide(rest, NY)
    return col_x, row_y, plane_z


def onehot(ids, size):
    tile = min(256, size)
    count = lax.broadcasted_iota(jnp.int32, (tile, ids.shape[1]), 0).astype(jnp.bfloat16)
    one = jnp.ones(count.shape, jnp.bfloat16)
    zero = jnp.zeros(count.shape, jnp.bfloat16)
    tiles = []
    for start in range(0, size, tile):
        here = jnp.broadcast_to((ids - start).astype(jnp.bfloat16), count.shape)
        tiles.append(jnp.where(count == here, one, zero))
    return jnp.concatenate(tiles, axis=0) if len(tiles) > 1 else tiles[0]


def fused_kernel(
    mol, grid, scale, cell_ref, move_ref, accept_ref, type_ref, table_ref,
    out_ref, own_ref,
    ids, total, count, inbox, fields, turned, part, inbox_e,
    send_a, recv_a, send_b, recv_b, send_e, recv_e,
):
    me = lax.axis_index("mol")
    slab = lax.axis_index("grid")
    beads = cell_ref.shape[1]
    blocks, block = part.shape[1], part.shape[3]
    planes = ZDEV * grid
    band = NY // mol
    half = count.shape[2] // 2

    barrier = pltpu.get_barrier_semaphore()
    for away in range(1, mol):
        pl.semaphore_signal(
            barrier, inc=1, device_id={"mol": lax.rem(me + away, mol)}, device_id_type=MESH
        )
    for away in range(1, grid):
        pl.semaphore_signal(
            barrier, inc=1, device_id={"grid": lax.rem(slab + away, grid)}, device_id_type=MESH
        )

    def window(index):
        return pl.ds(pl.multiple_of(index * block, block), block)

    def row_of(spot, kinds):
        _, row_y, plane_z = spot
        owner, row_here = divide(row_y, band)
        owner_z, plane_here = divide(plane_z, ZDEV)
        row = ((owner * TYPES + kinds) * band + row_here) * ZDEV + plane_here
        return jnp.where(owner_z == slab, row, -1)

    def wrap(value, length):
        value = jnp.where(value < 0, value + length, value)
        return jnp.where(value >= length, value - length, value)

    def begin_ids(index, carry):
        here = window(index)
        position = split_cell(cell_ref[:, here])
        ids[0, :, here] = row_of(position, type_ref[:, here])
        ids[1, :, here] = position[0]
        return carry

    def prepare(index, carry):
        here = window(index)
        kinds = type_ref[:, here]
        position = split_cell(cell_ref[:, here])
        for step in range(STEPS):
            lengths = (NX, NY, planes)
            proposed = tuple(
                wrap(position[i] + move_ref[i, step : step + 1, here], lengths[i]) for i in range(3)
            )
            if step > 0:
                ids[4 * step, :, here] = row_of(position, kinds)
                ids[4 * step + 1, :, here] = position[0]
            ids[4 * step + 2, :, here] = row_of(proposed, kinds)
            ids[4 * step + 3, :, here] = proposed[0]
            taken = accept_ref[step : step + 1, here] == 1
            position = tuple(jnp.where(taken, proposed[i], position[i]) for i in range(3))
        return carry

    lax.fori_loop(0, blocks, begin_ids, 0)

    def deposit(step, begin, end):
        def add(index, carry):
            here = window(index)
            rows = onehot(ids[4 * step, :, here], total.shape[0]).astype(jnp.float8_e4m3fn)
            cols = onehot(ids[4 * step + 1, :, here], total.shape[1]).astype(jnp.float8_e4m3fn)
            total[...] += lax.dot_general(
                rows, cols, (((1,), (1,)), ((), ())), preferred_element_type=jnp.float32
            )
            return carry

        if begin == 0:
            total[...] = jnp.zeros_like(total)
        lax.fori_loop(begin, end, add, 0)
        if end == blocks:
            count[step] = total[...].astype(jnp.bfloat16).reshape(count.shape[1:])

    def copy_a(step, away):
        to = lax.rem(me + away, mol)
        return pltpu.make_async_remote_copy(
            src_ref=count.at[step, to],
            dst_ref=inbox.at[step, away - 1],
            send_sem=send_a.at[step, away - 1],
            recv_sem=recv_a.at[step, away - 1],
            device_id={"mol": to},
            device_id_type=MESH,
        )

    partner = me + 1 - 2 * lax.rem(me, 2)
    chips = mol // 2

    def copy_b(step, index):
        if index == 0:
            slot, to = me, partner
        elif index < chips:
            slot, to = me, lax.rem(me + 2 * index, mol)
        else:
            slot, to = lax.rem(me + mol - 2 * (index - chips + 1), mol), partner
        return pltpu.make_async_remote_copy(
            src_ref=fields.at[step, slot],
            dst_ref=fields.at[step, slot],
            send_sem=send_b.at[step, index],
            recv_sem=recv_b.at[step, index],
            device_id={"mol": to},
            device_id_type=MESH,
        )

    def forward(step):
        for index in range(1, chips):
            copy_b(step, index).wait_recv()
            copy_b(step, index + chips - 1).start()

    def copy_e(step, index, away):
        return pltpu.make_async_remote_copy(
            src_ref=part.at[step, index],
            dst_ref=inbox_e.at[away - 1, step, index],
            send_sem=send_e.at[step, index, away - 1],
            recv_sem=recv_e.at[step, index, away - 1],
            device_id={"grid": lax.rem(slab + away, grid)},
            device_id_type=MESH,
        )

    def make_field(step):
        summed = count[step, me].astype(jnp.float32)
        for away in range(1, mol):
            copy_a(step, away).wait_recv()
            summed = summed + inbox[step, away - 1].astype(jnp.float32)
        high = summed.astype(jnp.bfloat16)
        low = (summed - high.astype(jnp.float32)).astype(jnp.bfloat16)
        table = table_ref[...]
        density = jnp.dot(high, table, preferred_element_type=jnp.float32)
        density = scale * (density + jnp.dot(low, table, preferred_element_type=jnp.float32))
        phi_a, phi_b = density[:half], density[half:]
        excess = kappa_comp * (phi_a + phi_b - 1.0)
        wide_a = chi_mix * phi_b + excess
        wide_b = chi_mix * phi_a + excess
        fields[step, me, :half] = wide_a.astype(jnp.bfloat16)
        fields[step, me, half:] = wide_b.astype(jnp.bfloat16)
        for index in reversed(range(chips)):
            copy_b(step, index).start()
        if step == STEPS - 1:
            for row in range(band):
                here = slice(row * ZDEV, (row + 1) * ZDEV)
                own_ref[row, :, :NX] = wide_a[here].astype(jnp.bfloat16)
                own_ref[row, :, NX:] = wide_b[here].astype(jnp.bfloat16)

    def turn(step):
        for index in [0, *range(chips, 2 * chips - 1)]:
            copy_b(step, index).wait_recv()
        eye = (
            lax.broadcasted_iota(jnp.int32, (NX, NX), 0)
            == lax.broadcasted_iota(jnp.int32, (NX, NX), 1)
        )
        eye = jnp.where(eye, 1.0, 0.0).astype(jnp.bfloat16)
        flat = fields[step].reshape(turned.shape[1], NX)
        turned[...] = lax.dot_general(
            eye, flat, (((1,), (1,)), ((), ())), preferred_element_type=jnp.float32
        ).astype(jnp.bfloat16)

    def pick(rows, cols):
        table = turned[...]
        values = jnp.dot(table, onehot(rows, table.shape[1]), preferred_element_type=jnp.float32)
        columns = lax.broadcasted_iota(jnp.int32, values.shape, 0)
        return jnp.sum(jnp.where(columns == cols, values, 0.0), axis=0, keepdims=True)

    def read(step, begin, end):
        def look(index, carry):
            here = window(index)
            old = pick(ids[4 * step, :, here], ids[4 * step + 1, :, here])
            new = pick(ids[4 * step + 2, :, here], ids[4 * step + 3, :, here])
            part[step, index] = new - old
            for away in range(1, grid):
                copy_e(step, index, away).start()
            return carry

        lax.fori_loop(begin, end, look, 0)

    deposit(0, 0, blocks)
    pl.semaphore_wait(barrier, mol - 1 + grid - 1)
    for away in range(1, mol):
        copy_a(0, away).start()
    lax.fori_loop(0, blocks, prepare, 0)
    deposit(1, 0, blocks)
    make_field(0)
    for away in range(1, mol):
        copy_a(1, away).start()
    forward(0)
    turn(0)
    middle, late = blocks // 4, blocks * 3 // 4
    read(0, 0, middle)
    make_field(1)
    read(0, middle, late)
    forward(1)
    read(0, late, blocks)
    turn(1)
    read(1, 0, blocks)

    for step in range(STEPS):
        def settle(index, carry):
            energy = part[step, index]
            for away in range(1, grid):
                copy_e(step, index, away).wait_recv()
                energy = energy + inbox_e[away - 1, step, index]
            out_ref[step : step + 1, window(index)] = energy
            return carry

        lax.fori_loop(0, blocks, settle, 0)
    for step in range(STEPS):
        for away in range(1, mol):
            copy_a(step, away).wait_send()
            copy_b(step, away - 1).wait_send()

        def drain(index, carry):
            for away in range(1, grid):
                copy_e(step, index, away).wait_send()
            return carry

        lax.fori_loop(0, blocks, drain, 0)


def local(cells_start, moves, accepted, bead_types):
    grid = lax.axis_size("grid")
    mol = lax.axis_size("mol")
    planes = ZDEV * grid
    beads = cells_start.shape[0]
    scale = NX * NY * planes / (beads * mol)
    band = NY // mol
    row_total = TYPES * NY * ZDEV
    rows = row_total // mol
    block = min(2048, beads)
    blocks = beads // block
    spec = pl.BlockSpec(memory_space=VMEM)
    bf16, f32 = jnp.bfloat16, jnp.float32
    dma = pltpu.SemaphoreType.DMA
    total, own = pl.pallas_call(
        functools.partial(fused_kernel, mol, grid, scale),
        out_shape=[
            jax.ShapeDtypeStruct((STEPS, beads), f32),
            jax.ShapeDtypeStruct((band, ZDEV, TYPES * NX), bf16),
        ],
        in_specs=[spec] * 5,
        out_specs=[spec] * 2,
        scratch_shapes=[
            pltpu.VMEM((4 * STEPS, 1, beads), jnp.int32),
            pltpu.VMEM((row_total, NX), f32),
            pltpu.VMEM((STEPS, mol, rows, NX), bf16),
            pltpu.VMEM((STEPS, mol - 1, rows, NX), bf16),
            pltpu.VMEM((STEPS, mol, rows, NX), bf16),
            pltpu.VMEM((NX, row_total), bf16),
            pltpu.VMEM((STEPS, blocks, 1, block), f32),
            pltpu.VMEM((grid - 1, STEPS, blocks, 1, block), f32),
            dma((STEPS, mol - 1)),
            dma((STEPS, mol - 1)),
            dma((STEPS, mol - 1)),
            dma((STEPS, mol - 1)),
            dma((STEPS, blocks, grid - 1)),
            dma((STEPS, blocks, grid - 1)),
        ],
        compiler_params=pltpu.CompilerParams(
            collective_id=0, has_side_effects=True, vmem_limit_bytes=LIMIT
        ),
        name="chain",
    )(
        cells_start.reshape(1, beads), moves.transpose(1, 0, 2), accepted,
        bead_types.reshape(1, beads), jnp.asarray(kernel_table()),
    )
    return total, own


def solution(mesh):
    return jax.shard_map(
        local,
        mesh=mesh,
        in_specs=(P("mol"), P(None, None, "mol"), P(None, "mol"), P("mol")),
        out_specs=(P(None, "mol"), P("mol", "grid", None)),
        check_vma=False,
    )
```
